128 devices in a mesh: dp: 16 (over y_hi, z, core), vocab: 8 (over x, y_lo).
Axes of the slice: x: 4, y: 4 (y_hi: 2, y_lo: 2; y = y_hi * 2 + y_lo), z: 4, core: 2. Of those that a mesh axis runs over, the one named last changes fastest.
Arguments:
- hidden: bfloat16 [768, 5120], P('dp')
- head_weight: bfloat16 [131072, 5120], P(('dp', 'vocab'))
- target_ids: int32 [768], P('dp'), may hold values from 0 to 131071
- response_mask: int32 [768], P('dp'), may hold values 0 or 1
- advantages: bfloat16 [768], P('dp'), may hold values from -0.23925781 to 0.23925781
- seq_tokens: int32 [128], P('dp'), may hold values from 24 to 144
- layer_grads: float32 [16, 1024, 8192], P('dp', None, 'vocab'), may hold values from -3 to 3
Outputs:
- grad_hidden: bfloat16 [768, 5120], P('dp', 'vocab')
- grad_weight: bfloat16 [131072, 5120], P(('dp', 'vocab'))
- reduced_bucket: float32 [1024, 8192], P('dp', 'vocab')
The draws below stay inside these ranges and needn't reach their ends.
All inputs are finite; a program needn't handle non-finite values. No bound on the sum of `response_mask` on one device may be relied on, other than what follows from the above.
Results may differ from the reference program's by a relative error of at most 0.015.
Values may be sent and summed in bfloat16 or wider, within the bound.
No kernel may reach another device: no remote copies, remote signals or barrier semaphores. Data moves between devices by JAX's collectives and lax.ppermute only.
A program may use at most 192 MiB of HBM per device.

```python
import math
import jax
import jax.numpy as jnp
from jax import lax

D = 5120
VOC_DEV = 1024
TOK_DEV = 48
BK_COLS = 1024
TOKENS = 768
VOCAB = 131072
SEQS = 128
BK_ROWS = 1024
N_DP = 16
N_VOCAB = 8


def head_rows(weight_key, row_ids):

    def single_row(row_index):
        values = jax.random.normal(jax.random.fold_in(weight_key, row_index), (D,), jnp.float32)
        return jnp.clip(values, -6.0, 6.0) * (3.0 / math.sqrt(D))
    return jax.vmap(single_row)(row_ids)


def draw_head_weight(key, part):
    weight_key = jax.random.fold_in(key, 11)
    row_ids = jnp.arange(VOCAB, dtype=jnp.int32).reshape(VOCAB // VOC_DEV, VOC_DEV)
    blocks = lax.map(lambda block_ids: head_rows(weight_key, block_ids).astype(jnp.bfloat16), row_ids)
    return blocks.reshape(VOCAB, D)


def peaked_rows(key, weight_key):
    shard_count = VOCAB // VOC_DEV
    peak_count = min(shard_count, D // 8)
    peak_shards = jnp.arange(peak_count, dtype=jnp.int32) * shard_count // peak_count
    key_offset, key_height = jax.random.split(jax.random.fold_in(key, 31), 2)
    offsets = jax.random.randint(key_offset, (TOKENS, peak_count), 0, VOC_DEV, dtype=jnp.int32)
    peak_ids = peak_shards[None, :] * VOC_DEV + offsets
    heights = 9.0 + jax.random.uniform(key_height, (TOKENS, peak_count), jnp.float32, -1.0, 1.0)

    def one_token(packed):
        peak_rows, peak_height = packed
        head_block = head_rows(weight_key, peak_rows).astype(jnp.bfloat16).astype(jnp.float32)
        gram_matrix = jnp.dot(head_block, head_block.T, precision=lax.Precision.HIGHEST)
        ridge_term = 0.05 * jnp.mean(jnp.diagonal(gram_matrix))
        identity = jnp.eye(peak_count, dtype=jnp.float32)
        coefficients = jnp.linalg.solve(gram_matrix + ridge_term * identity, peak_height)
        return jnp.dot(coefficients, head_block, precision=lax.Precision.HIGHEST)
    return lax.map(one_token, (peak_ids, heights))


def draw_hidden(key, part):
    weight_key = jax.random.fold_in(key, 11)
    hidden_key = jax.random.fold_in(key, 23)
    noise = jnp.clip(jax.random.normal(hidden_key, (TOKENS, D), jnp.float32), -6.0, 6.0)
    values = peaked_rows(key, weight_key) + 0.15 * noise
    values = jnp.clip(values, -6.0, 6.0)
    return values.astype(jnp.bfloat16)


def draw_seq_tokens(key, part):
    position = jnp.arange(SEQS, dtype=jnp.int32)
    centre = TOK_DEV * (SEQS - 1 + 2 * position) // (SEQS - 1)
    key_vals, key_high, key_low = jax.random.split(jax.random.fold_in(key, 37), 3)
    counts = jax.random.randint(key_vals, (SEQS,), centre // 2, centre + 1, dtype=jnp.int32)
    half = SEQS // 2
    high_pos = jax.random.randint(key_high, (), half, SEQS, dtype=jnp.int32)
    low_pos = jax.random.randint(key_low, (), 0, half, dtype=jnp.int32)
    counts = jnp.where(position == high_pos, 3 * TOK_DEV, counts)
    counts = jnp.where(position == low_pos, TOK_DEV // 2, counts)
    return counts.astype(jnp.int32)


def touch_ends(entries, stream_key, smallest, largest):
    spot = [jax.random.randint(jax.random.fold_in(stream_key, axis), (), 0, length) for axis, length in enumerate(entries.shape)]
    widest = entries.shape.index(max(entries.shape))
    next_to = spot[:widest] + [(spot[widest] + 1) % entries.shape[widest]] + spot[widest + 1:]
    return entries.at[tuple(spot)].set(smallest).at[tuple(next_to)].set(largest)


def spiked(values, stream_key, source, target, blocks, factor):
    def block_of(dim):
        return (jnp.arange(values.shape[dim]) // (values.shape[dim] // blocks)).reshape((-1,) + (1,) * (values.ndim - 1 - dim))

    one_side = jax.random.permutation(stream_key, blocks)[block_of(target)]
    far = (block_of(target) + blocks // 2) % blocks
    return jnp.where((block_of(source) == one_side) | (block_of(source) == far), factor * values, values)


def steps_of(key, shape, shards, least, largest):
    level, own = 1.0, jax.random.fold_in(key, 6)
    for dim, shards_of in shards:
        steps = jnp.exp(jax.random.uniform(jax.random.fold_in(own, dim), (shards_of,), jnp.float32, least / len(shards), largest / len(shards)))
        level = level * jnp.repeat(steps, shape[dim] // shards_of).reshape([-1 if axis == dim else 1 for axis in range(len(shape))])
    return level


def gaussian(rng, dims, spread, reach, shards=(), held_as=jnp.bfloat16):
    entries = spread * jax.random.normal(rng, dims, jnp.float32)
    if shards:
        entries = entries * steps_of(rng, dims, shards, -0.22, 0.18)
    return jnp.clip(entries, -reach, reach).astype(held_as)


def noise_with(own_key, dims, spread, reach, cuts, heavy, kind=jnp.bfloat16):
    values = spread * jax.random.normal(own_key, dims, jnp.float32)
    if cuts:
        values = values * steps_of(own_key, dims, cuts, -0.22, 0.18)
    return jnp.clip(spiked(values, jax.random.fold_in(own_key, 3), *heavy), -reach, reach).astype(kind)


def setup_inputs(seed: int = 0) -> dict:
    key_of = jax.random.split(jax.random.key(seed), 8)
    hidden = draw_hidden(jax.random.fold_in(key_of[7], 71), 0)
    head_weight = draw_head_weight(jax.random.fold_in(key_of[7], 71), 0)
    target_ids = touch_ends(jax.random.randint(key_of[2], (TOKENS,), 0, VOCAB), jax.random.fold_in(key_of[2], 1), 0, VOCAB - 1).astype(jnp.int32)
    response_mask = touch_ends((jax.random.randint(key_of[3], (TOKENS,), 0, 4) < 3).astype(jnp.int32), jax.random.fold_in(key_of[3], 1), 0, 1)
    advantages = gaussian(key_of[4], (TOKENS,), 0.04, 0.23925781, ((0, 16),))
    seq_tokens = draw_seq_tokens(jax.random.fold_in(key_of[7], 71), 0)
    layer_grads = noise_with(key_of[6], (N_DP, BK_ROWS, BK_COLS * N_VOCAB), 0.25, 3.0, ((0, 16), (2, 8)), (0, 1, 16, 2.0), jnp.float32)
    return {"hidden": hidden, "head_weight": head_weight, "target_ids": target_ids, "response_mask": response_mask, "advantages": advantages, "seq_tokens": seq_tokens, "layer_grads": layer_grads}


loss_scale = 16.0
entropy_coef = 0.1

def combine_stats(first, second):
    first_max, first_sum, first_ent, first_tgt = first
    second_max, second_sum, second_ent, second_tgt = second
    joint_max = jnp.maximum(first_max, second_max)
    first_f = jnp.exp(first_max - joint_max)
    second_f = jnp.exp(second_max - joint_max)
    return (joint_max, first_sum * first_f + second_sum * second_f, first_ent * first_f + second_ent * second_f, first_tgt + second_tgt)

def reference(hidden, head_weight, target_ids, response_mask, advantages, seq_tokens, layer_grads):
    num_blocks = head_weight.shape[0] // VOC_DEV
    w_blocks = head_weight.reshape(num_blocks, VOC_DEV, D)
    offsets = jnp.arange(num_blocks, dtype=jnp.int32) * VOC_DEV
    local_rows = jnp.arange(VOC_DEV, dtype=jnp.int32)[:, None]

    def logits_of(w_block):
        return jnp.dot(w_block.astype(jnp.float32), hidden.T.astype(jnp.float32), preferred_element_type=jnp.float32)

    def stats_step(running, packed):
        w_block, offset = packed
        logits = logits_of(w_block)
        block_max = jnp.max(logits, axis=0)
        shifted = jnp.exp(logits - block_max[None, :])
        onehot = offset + local_rows == target_ids[None, :]
        block = (block_max, jnp.sum(shifted, axis=0), jnp.sum(shifted * logits, axis=0), jnp.sum(jnp.where(onehot, logits, jnp.zeros_like(logits)), axis=0))
        return (combine_stats(running, block), None)
    tokens = hidden.shape[0]
    start_stats = (jnp.full((tokens,), -jnp.inf, dtype=jnp.float32), jnp.zeros((tokens,), jnp.float32), jnp.zeros((tokens,), jnp.float32), jnp.zeros((tokens,), jnp.float32))
    (row_max, row_sum, row_ent, row_tgt), _ = lax.scan(stats_step, start_stats, (w_blocks, offsets))
    token_total = jnp.sum(seq_tokens.astype(jnp.float32))
    factor = loss_scale * tokens / token_total
    weights = factor * response_mask.astype(jnp.float32)
    advantage = advantages.astype(jnp.float32)
    mean_logit = row_ent / row_sum

    def grad_step(accum, packed):
        w_block, offset = packed
        logits = logits_of(w_block)
        softmax = jnp.exp(logits - row_max[None, :]) / row_sum[None, :]
        onehot = (offset + local_rows == target_ids[None, :]).astype(jnp.float32)
        logit_grad = weights[None, :] * (-advantage[None, :] * (onehot - softmax) + entropy_coef * softmax * (logits - mean_logit[None, :]))
        grad_bf = logit_grad.astype(jnp.bfloat16)
        weight_grad = jnp.dot(grad_bf.astype(jnp.float32), hidden.astype(jnp.float32), preferred_element_type=jnp.float32).astype(jnp.bfloat16)
        accum = accum + jnp.dot(grad_bf.T.astype(jnp.float32), w_block.astype(jnp.float32), preferred_element_type=jnp.float32)
        return (accum, weight_grad)
    grad_sum, weight_grads = lax.scan(grad_step, jnp.zeros((tokens, D), jnp.float32), (w_blocks, offsets))
    grad_hidden = grad_sum.astype(jnp.bfloat16)
    grad_weight = weight_grads.reshape(head_weight.shape[0], D)
    reduced_bucket = jnp.sum(layer_grads, axis=0) * factor
    return (grad_hidden, grad_weight, reduced_bucket)
```

```python
import jax
import jax.numpy as jnp
from jax import lax
from jax.experimental import pallas as pl
from jax.experimental.pallas import tpu as pltpu
from jax.sharding import Mesh
from jax.sharding import PartitionSpec as P

DP = ("dp_0", "dp_1", "dp_2")
VOCAB = ("vocab_0", "vocab_1")
DP_VOCAB = DP + VOCAB
DP_CHIPS = ("dp_0", "dp_1")
CHIPS = DP_CHIPS + VOCAB

loss_scale = 16.0
entropy_coef = 0.1


VOC_BLOCK = 256


def exchange(array, axes):
    return lax.all_to_all(array, axes, 0, 0, tiled=True)


def spread(array, axes):
    members = lax.axis_size(axes)
    return exchange(jnp.broadcast_to(array[None], (members, *array.shape)), axes)


def other_core(array):
    return lax.ppermute(array, "dp_2", [(0, 1), (1, 0)])


def f32(array):
    return array.astype(jnp.float32)


def bf16(array):
    return array.astype(jnp.bfloat16)


def assemble_kernel(source, out):
    out[...] = source[...].reshape(out.shape)


def assembled(array):
    chips, blocks, rows, cols = array.shape
    return pl.pallas_call(
        assemble_kernel,
        grid=(blocks,),
        in_specs=[pl.BlockSpec((chips, 1, rows, cols), lambda j: (0, j, 0, 0))],
        out_specs=pl.BlockSpec((chips * rows, cols), lambda j: (0, j)),
        out_shape=jax.ShapeDtypeStruct((chips * rows, blocks * cols), array.dtype),
        name="assemble",
    )(array)


def logits_kernel(weight, hidden, logits, stats):
    step = pl.program_id(0)
    block = lax.dot_general(
        weight[...], hidden[...], (((1,), (1,)), ((), ())), preferred_element_type=jnp.float32
    )
    logits[...] = block
    top = jnp.max(block, axis=0, keepdims=True)
    shifted = jnp.exp(block - top)
    total = jnp.sum(shifted, axis=0, keepdims=True)
    ent = jnp.sum(shifted * block, axis=0, keepdims=True)

    @pl.when(step == 0)
    def _():
        stats[0:1, :] = top
        stats[1:2, :] = total
        stats[2:3, :] = ent

    @pl.when(step > 0)
    def _():
        old = stats[0:1, :]
        joint = jnp.maximum(old, top)
        old_f, new_f = jnp.exp(old - joint), jnp.exp(top - joint)
        stats[0:1, :] = joint
        stats[1:2, :] = stats[1:2, :] * old_f + total * new_f
        stats[2:3, :] = stats[2:3, :] * old_f + ent * new_f


def local_logits(weight, hidden):
    voc, width = weight.shape
    tokens = hidden.shape[0]
    return pl.pallas_call(
        logits_kernel,
        grid=(voc // VOC_BLOCK,),
        in_specs=[
            pl.BlockSpec((VOC_BLOCK, width), lambda i: (i, 0)),
            pl.BlockSpec((tokens, width), lambda i: (0, 0)),
        ],
        out_specs=(
            pl.BlockSpec((VOC_BLOCK, tokens), lambda i: (i, 0)),
            pl.BlockSpec((3, tokens), lambda i: (0, 0)),
        ),
        out_shape=(
            jax.ShapeDtypeStruct((voc, tokens), jnp.float32),
            jax.ShapeDtypeStruct((3, tokens), jnp.float32),
        ),
        cost_estimate=pl.CostEstimate(
            flops=2 * voc * tokens * width,
            bytes_accessed=2 * (voc + tokens) * width,
            transcendentals=voc * tokens,
        ),
        name="logits",
    )(weight, hidden)


def grad_kernel(first_id, logits, table, grad, turned):
    block = logits[...]
    ids = first_id[0] + pl.program_id(0) * block.shape[0]
    ids = ids + lax.broadcasted_iota(jnp.int32, block.shape, 0)
    label, weight, advantage = table[0:1, :], table[1:2, :], table[2:3, :]
    row_max, row_sum, mean_logit = table[3:4, :], table[4:5, :], table[5:6, :]
    softmax = jnp.exp(block - row_max) * (1.0 / row_sum)
    onehot = jnp.where(ids == label.astype(jnp.int32), 1.0, 0.0)
    value = weight * (
        -advantage * (onehot - softmax) + entropy_coef * softmax * (block - mean_logit)
    )
    grad[...] = value.astype(grad.dtype)
    turned[...] = value.T.astype(turned.dtype)


def logit_gradient(first_id, logits, table):
    voc, tokens = logits.shape
    return pl.pallas_call(
        grad_kernel,
        grid=(voc // VOC_BLOCK,),
        in_specs=[
            pl.BlockSpec(memory_space=pltpu.SMEM),
            pl.BlockSpec((VOC_BLOCK, tokens), lambda i: (i, 0)),
            pl.BlockSpec((6, tokens), lambda i: (0, 0)),
        ],
        out_specs=(
            pl.BlockSpec((VOC_BLOCK, tokens), lambda i: (i, 0)),
            pl.BlockSpec((tokens, VOC_BLOCK), lambda i: (0, i)),
        ),
        out_shape=(
            jax.ShapeDtypeStruct((voc, tokens), jnp.bfloat16),
            jax.ShapeDtypeStruct((tokens, voc), jnp.bfloat16),
        ),
        cost_estimate=pl.CostEstimate(
            flops=10 * voc * tokens, bytes_accessed=8 * voc * tokens, transcendentals=voc * tokens
        ),
        name="logit_gradient",
    )(first_id, logits, table)


def other_kernel(turned, weight, out):
    out[...] = jnp.dot(turned[...], weight[...], preferred_element_type=jnp.float32).astype(
        out.dtype
    )


def own_kernel(turned, weight, received, out):
    part = jnp.dot(turned[...], weight[...], preferred_element_type=jnp.float32)
    out[...] = (part + received[...].astype(jnp.float32)).astype(out.dtype).reshape(out.shape)


def hidden_terms(turned, weight, blocks, received=None, chips=None):
    tokens, voc = turned.shape
    width = weight.shape[1]
    cols = width // blocks
    in_specs = [
        pl.BlockSpec((tokens, voc), lambda j: (0, 0)),
        pl.BlockSpec((voc, cols), lambda j: (0, j)),
    ]
    cost = pl.CostEstimate(
        flops=2 * voc * tokens * width, bytes_accessed=2 * (voc + tokens) * width, transcendentals=0
    )
    if received is None:
        return pl.pallas_call(
            other_kernel,
            grid=(blocks,),
            in_specs=in_specs,
            out_specs=pl.BlockSpec((tokens, cols), lambda j: (0, j)),
            out_shape=jax.ShapeDtypeStruct((tokens, width), jnp.bfloat16),
            cost_estimate=cost,
            name="hidden_other",
        )(turned, weight)
    rows = tokens // chips
    return pl.pallas_call(
        own_kernel,
        grid=(blocks,),
        in_specs=[*in_specs, pl.BlockSpec((tokens, cols), lambda j: (0, j))],
        out_specs=pl.BlockSpec((chips, 1, rows, cols), lambda j: (0, j, 0, 0)),
        out_shape=jax.ShapeDtypeStruct((chips, blocks, rows, cols), jnp.bfloat16),
        cost_estimate=cost,
        name="hidden_own",
    )(turned, weight, received)


def weight_kernel(own_grad, own_hidden, other_grad, other_hidden, *refs):
    out = refs[-1]
    own = jnp.dot(own_grad[...], own_hidden[...], preferred_element_type=jnp.float32)
    other = jnp.dot(other_grad[...], other_hidden[...], preferred_element_type=jnp.float32)
    out[...] = (own + other).astype(out.dtype)


def weight_gradient(grads, hiddens, blocks, start, stop, earlier=None):
    voc, tokens = grads[0].shape
    width = hiddens[0].shape[1]
    cols = width // blocks
    grad_spec = pl.BlockSpec((voc, tokens), lambda j: (0, 0))
    hidden_spec = pl.BlockSpec((tokens, cols), lambda j: (0, start + j))
    kept = () if earlier is None else (earlier,)
    part = (stop - start) * cols
    return pl.pallas_call(
        weight_kernel,
        grid=(stop - start,),
        in_specs=[grad_spec, hidden_spec] * 2 + [pl.BlockSpec(memory_space=pl.ANY)] * len(kept),
        out_specs=pl.BlockSpec((voc, cols), lambda j: (0, start + j)),
        out_shape=jax.ShapeDtypeStruct((voc, width), jnp.bfloat16),
        input_output_aliases={} if earlier is None else {4: 0},
        cost_estimate=pl.CostEstimate(
            flops=4 * voc * tokens * part,
            bytes_accessed=2 * (voc + 2 * tokens) * part,
            transcendentals=0,
        ),
        name="weight_gradient",
    )(grads[0], hiddens[0], grads[1], hiddens[1], *kept)


def merged(stats):
    top = jnp.max(stats[:, 0], axis=0)
    scale = jnp.exp(stats[:, 0] - top[None])
    return jnp.stack(
        [top, jnp.sum(stats[:, 1] * scale, axis=0), jnp.sum(stats[:, 2] * scale, axis=0)]
    )


def on_device(hidden, head_weight, target_ids, response_mask, advantages, seq_tokens, layer_grads):
    vocab_count = lax.axis_size(VOCAB)
    tok_rows, width = hidden.shape
    voc_rows = head_weight.shape[0]
    cols = width // vocab_count
    replicas = lax.axis_size(DP)
    tokens = replicas * tok_rows
    half = tokens // 2
    chips = replicas // 2
    core = lax.axis_index("dp_2")

    piece = lax.dynamic_slice(
        hidden, (0, lax.axis_index(VOCAB) * cols), (tok_rows, cols)
    )
    own_hidden = assembled(spread(piece, CHIPS).reshape(chips, vocab_count, tok_rows, cols))
    other_hidden = other_core(own_hidden)

    count = jnp.broadcast_to(jnp.sum(seq_tokens).astype(jnp.float32), (tok_rows,))
    small = jnp.stack([f32(target_ids), f32(response_mask), f32(advantages), count])
    small = spread(small, DP)
    token_total = jnp.sum(small[:, 3, 0])
    factor = loss_scale * tokens / token_total
    small = small[:, :3].reshape(chips, 2, 3, tok_rows).transpose(2, 1, 0, 3).reshape(3, 2, half)
    small = jnp.where(core == 0, small, small[:, ::-1])

    own_logits, own_stats = local_logits(head_weight, own_hidden)
    other_logits, other_stats = local_logits(head_weight, other_hidden)

    bucket = layer_grads[0].reshape(chips, 2, -1, layer_grads.shape[2])
    given = bf16(jnp.where(core == 0, bucket[:, 1], bucket[:, 0]))
    kept = bf16(jnp.where(core == 0, bucket[:, 0], bucket[:, 1]))
    given, kept, _ = lax.optimization_barrier((given, kept, own_hidden))
    pair = bf16(f32(kept) + f32(other_core(given)))
    bucket_sum = jnp.sum(f32(exchange(pair, DP_CHIPS)), axis=0)

    stats = jnp.concatenate([own_stats, other_stats], axis=1)
    stats = merged(spread(stats, VOCAB))
    turned = jnp.concatenate([stats[:, half:], stats[:, :half]], axis=1)
    both = jnp.stack([jnp.where(core == 0, stats, turned), jnp.where(core == 0, turned, stats)])
    both = jnp.broadcast_to(both[None], (chips, *both.shape)).reshape(replicas, 3, tokens)
    row_max, row_sum, row_ent = merged(exchange(both, DP)).reshape(3, 2, half)

    first_id = (lax.axis_index(DP) * vocab_count + lax.axis_index(VOCAB)) * voc_rows
    first_id = first_id.astype(jnp.int32).reshape(1)
    table = jnp.stack([small[0], factor * small[1], small[2], row_max, row_sum, row_ent / row_sum])
    other_grad, other_turned = logit_gradient(first_id, other_logits, table[:, 1])
    own_grad, own_turned = logit_gradient(first_id, own_logits, table[:, 0])

    received = other_core(hidden_terms(other_turned, head_weight, vocab_count))
    grads, hiddens = (own_grad, other_grad), (own_hidden, other_hidden)
    first_half = weight_gradient(grads, hiddens, vocab_count, 0, vocab_count // 2)
    chip_terms = hidden_terms(own_turned, head_weight, vocab_count, received, chips)
    terms = exchange(chip_terms.reshape(chips * vocab_count, tok_rows, cols), CHIPS)
    grad_weight = weight_gradient(
        grads, hiddens, vocab_count, vocab_count // 2, vocab_count, first_half
    )
    grad_hidden = bf16(jnp.sum(f32(terms), axis=0))
    reduced_bucket = bucket_sum * factor
    return (grad_hidden, grad_weight, reduced_bucket)


def solution(mesh):
    split = Mesh(
        mesh.devices.reshape(2, 4, 2, 4, 2), ("dp_0", "dp_1", "dp_2", "vocab_0", "vocab_1")
    )
    return jax.shard_map(
        on_device,
        mesh=split,
        in_specs=(P(DP, None), P(DP_VOCAB, None), P(DP), P(DP), P(DP), P(DP), P(DP, None, VOCAB)),
        out_specs=(P(DP, VOCAB), P(DP_VOCAB, None), P(DP, VOCAB)),
        check_vma=False,
    )
```
